128 devices in a mesh: worker: 4 (over y_hi, core), outer: 4 (over x), mp: 8 (over y_lo, z).
Axes of the slice: x: 4, y: 4 (y_hi: 2, y_lo: 2; y = y_hi * 2 + y_lo), z: 4, core: 2. Of those that a mesh axis runs over, the one named last changes fastest.
Arguments:
- grads: float32 [4, 4, 3584, 4096], P('worker', 'outer', None, 'mp'), as said below
- center: float32 [3584, 4096], P(('worker', 'outer'), 'mp'), may hold values from -6 to 6
- radius: float32 [1], replicated, may hold values from 1.5 to 3.5
Outputs:
- center_out: float32 [3584, 4096], P(('worker', 'outer'), 'mp')
The draws below stay inside these ranges and needn't reach their ends.
Inputs may be any that keep to these rules, and one draw needn't show every extreme that they name: `grads`: finite values.
All inputs are finite; a program needn't handle non-finite values.
Results may differ from the reference program's by a relative error of at most 0.0001.
Values sent between devices are 32-bit elements; how exact they have to be, the bound alone decides.
A program may use at most 128 MiB of HBM per device.

```python
import math
import jax
import jax.numpy as jnp
from jax import lax

D = 3584
ITERS = 2
KVW = 4096
N_WORKER = 4
N_OUTER = 4


def draw_grads(key, part):
    keys = jax.random.split(key, 4)
    worker_scale = jnp.exp(jax.random.uniform(keys[0], (N_WORKER, N_OUTER, 1, 1), jnp.float32, math.log(0.4), math.log(4.0)))
    row_scale = jnp.exp(jax.random.uniform(keys[1], (1, 1, D, 1), jnp.float32, math.log(0.3), math.log(3.0)))
    columns = jnp.arange(KVW, dtype=jnp.float32) / KVW - 0.5
    trend = jnp.exp(math.log(3.0) * columns).reshape(1, 1, 1, KVW)
    column_scale = trend * jnp.exp(jax.random.uniform(keys[2], (1, 1, 1, KVW), jnp.float32, math.log(0.5), math.log(2.0)))
    shape = (N_WORKER, N_OUTER, D, KVW)
    noise = jax.random.normal(keys[3], shape, jnp.float32)
    return (worker_scale * row_scale * column_scale * noise).astype(jnp.float32)


def steps_of(own_key, dims, shards, smallest, top_value):
    factor_of, own = 1.0, jax.random.fold_in(own_key, 6)
    for position, shards_of in shards:
        steps = jnp.exp(jax.random.uniform(jax.random.fold_in(own, position), (shards_of,), jnp.float32, smallest / len(shards), top_value / len(shards)))
        factor_of = factor_of * jnp.repeat(steps, dims[position] // shards_of).reshape([-1 if axis == position else 1 for axis in range(len(dims))])
    return factor_of


def normal_values(stream_key, extent, deviation, most, pieces=(), held_as=jnp.bfloat16):
    result = jax.random.normal(stream_key, extent, jnp.float32) * deviation
    if len(pieces) > 0:
        result = steps_of(stream_key, extent, pieces, -0.22, 0.18) * result
    return jnp.clip(result, min=-most, max=most).astype(held_as)


def setup_inputs(seed: int = 0) -> dict:
    streams_of = jax.random.split(jax.random.key(seed), 4)
    grads = draw_grads(jax.random.fold_in(streams_of[3], 71), 0)
    center = normal_values(streams_of[1], (D, KVW), 1.0, 6.0, ((0, 16), (1, 8)), jnp.float32)
    radius = jnp.clip(jax.random.uniform(streams_of[2], (1,), jnp.float32, 1.5, 3.5), 1.5, 3.5)
    return dict(grads=grads, center=center, radius=radius)


epsilon = 1e-06

def reference(grads, center, radius):
    per_worker = grads.reshape(N_WORKER * N_OUTER, D, KVW)
    radius_total = radius[0] * math.sqrt(D * KVW)
    current = center
    for iteration in range(ITERS):

        def accumulate(summed, gradient):
            difference = gradient - current
            squares = jnp.sum(difference * difference)
            factor = jnp.minimum(1.0, radius_total * lax.rsqrt(squares + epsilon))
            return (summed + factor * difference, None)
        summed, unused = lax.scan(accumulate, jnp.zeros_like(center), per_worker)
        current = current + summed / (N_WORKER * N_OUTER)
    return current
```

```python
import functools
import math

import jax
import jax.numpy as jnp
from jax import lax
from jax.experimental import pallas as pl
from jax.experimental.pallas import tpu as pltpu
from jax.sharding import PartitionSpec as P

MESH = pl.DeviceIdType.MESH
D = 3584
KVW = 4096
WORKERS = 16
MP = 8
EPS = 1e-06
CHUNKS = 7
LANES = 128
BLOCK = 4


def send_order():
    order = []
    for core in (0, 1):
        for flip in (0, 1):
            for step in (1, 3, 2):
                order.append((flip, step, core))
            if core == 1:
                order.append((flip, 0, core))
    return order


def kernel(rows, chunk, grads, center, radius, out, held, start, acc, bias, mine, group, half, lines, sent, landed, near, scalar_sent, scalar_landed):
    w, o, m = lax.axis_index("worker"), lax.axis_index("outer"), lax.axis_index("mp")
    high, core = w // 2, w % 2
    me = w * 4 + o

    own = pltpu.make_async_copy(grads.at[pl.ds(pl.multiple_of(me * rows, 8), rows)], held.at[me], near.at[0])
    base = pltpu.make_async_copy(center, start, near.at[1])
    own.start()
    base.start()

    barrier = pltpu.get_barrier_semaphore()
    for k in range(1, WORKERS):
        pl.semaphore_signal(barrier, inc=1, device_id=((w + k // 4) % 4, (o + k % 4) % 4, m), device_id_type=MESH)
    for k in range(1, MP):
        pl.semaphore_signal(barrier, inc=1, device_id=(w, o, (m + k) % MP), device_id_type=MESH)
    pl.semaphore_wait(barrier, WORKERS + MP - 2)

    def send(c, carry):
        at = pl.multiple_of(c * chunk, 8)

        def to(worker, outer):
            target = worker * 4 + outer
            pltpu.make_async_remote_copy(
                src_ref=grads.at[pl.ds(pl.multiple_of(target * rows + at, 8), chunk)],
                dst_ref=held.at[me, pl.ds(at, chunk)],
                send_sem=sent,
                recv_sem=landed.at[c],
                device_id=(worker, outer, m),
                device_id_type=MESH,
            ).start()

        to(((high + 1) % 2) * 2 + core, o)
        for flip, step, other in send_order():
            to(((high + flip + core) % 2) * 2 + (core + other) % 2, (o + step) % 4)
        return carry

    lax.fori_loop(0, CHUNKS, send, 0)

    acc[...] = jnp.zeros_like(acc)
    own.wait()
    base.wait()

    def gather(c, carry):
        at = pl.multiple_of(c * chunk, 8)
        arrived = held.at[pl.ds(0, WORKERS - 1), pl.ds(at, chunk)]
        pltpu.make_async_copy(arrived, arrived, landed.at[c]).wait()

        def subtract(t, carry):
            here = pl.ds(pl.multiple_of(at + t * 8, 8), 8)
            v = start[here, :]
            for i in range(WORKERS):
                held[i, here, :] = held[i, here, :] - v
            return carry

        lax.fori_loop(0, chunk // 8, subtract, 0)
        for bi in range(WORKERS // BLOCK):
            for bj in range(bi, WORKERS // BLOCK):
                pairs = [(i, j) for i in range(bi * BLOCK, (bi + 1) * BLOCK) for j in range(bj * BLOCK, (bj + 1) * BLOCK) if i <= j]

                def products(t, sums, bi=bi, bj=bj, pairs=pairs):
                    here = pl.ds(pl.multiple_of(at + t * 8, 8), 8)
                    sums = list(sums)
                    for q in range(held.shape[2] // LANES):
                        there = slice(q * LANES, (q + 1) * LANES)
                        d = {i: held[i, here, there] for i in range(bi * BLOCK, (bi + 1) * BLOCK)}
                        for j in range(bj * BLOCK, (bj + 1) * BLOCK):
                            if j not in d:
                                d[j] = held[j, here, there]
                        for k, (i, j) in enumerate(pairs):
                            sums[k] = sums[k] + d[i] * d[j]
                    return tuple(sums)

                sums = lax.fori_loop(0, chunk // 8, products, tuple(acc[i * WORKERS + j] for i, j in pairs))
                for (i, j), total in zip(pairs, sums, strict=True):
                    acc[i * WORKERS + j] = total
        return carry

    lax.fori_loop(0, CHUNKS, gather, 0)

    for i in range(WORKERS):
        at = (i // 8) * LANES + ((8 - i % 8) % 8) * WORKERS
        for j in range(WORKERS):
            lines[at + j : at + j + 1, :] = jnp.sum(acc[min(i, j) * WORKERS + max(i, j)], axis=0, keepdims=True)
    across = lax.dot_general(
        jnp.full((8, LANES), 1.0, jnp.float32),
        lines[...] * 0.0625,
        (((1,), (1,)), ((), ())),
        precision=lax.Precision.HIGHEST,
        preferred_element_type=jnp.float32,
    )
    top = lax.broadcasted_iota(jnp.int32, (8, LANES), 0) == 0
    mine[...] = jnp.where(top, across[:, :LANES], across[:, LANES:]) * 16.0

    for k in range(1, WORKERS):
        pltpu.make_async_remote_copy(
            src_ref=mine, dst_ref=group.at[me], send_sem=scalar_sent.at[0], recv_sem=scalar_landed.at[0],
            device_id=((w + k // 4) % 4, (o + k % 4) % 4, m), device_id_type=MESH,
        ).start()
    group[me] = mine[...]
    arrived = group.at[pl.ds(0, WORKERS - 1)]
    pltpu.make_async_copy(arrived, arrived, scalar_landed.at[0]).wait()
    part = jnp.sum(group[...], axis=0)
    half[MP] = part
    for k in range(1, MP):
        pltpu.make_async_remote_copy(
            src_ref=half.at[MP], dst_ref=half.at[m], send_sem=scalar_sent.at[1], recv_sem=scalar_landed.at[1],
            device_id=(w, o, (m + k) % MP), device_id_type=MESH,
        ).start()
    half[m] = part
    pltpu.make_async_copy(held.at[pl.ds(0, WORKERS - 1)], held.at[pl.ds(0, WORKERS - 1)], sent).wait()
    pltpu.make_async_copy(arrived, arrived, scalar_sent.at[0]).wait()
    arrived = half.at[pl.ds(0, MP - 1)]
    pltpu.make_async_copy(arrived, arrived, scalar_landed.at[1]).wait()
    pltpu.make_async_copy(arrived, arrived, scalar_sent.at[1]).wait()
    total = jnp.sum(half[0:MP], axis=0)

    tables = [
        pltpu.roll(jnp.broadcast_to(total[h : h + 1, :], (8, LANES)), 0, 1, stride=WORKERS, stride_axis=0) for h in (0, 1)
    ]
    gram = jnp.concatenate(tables, axis=0)
    row = lax.broadcasted_iota(jnp.int32, (WORKERS, LANES), 0)
    column = lax.broadcasted_iota(jnp.int32, (WORKERS, LANES), 1)
    tau = radius[0] * math.sqrt(D * KVW)

    def share(squares):
        return jnp.minimum(1.0, tau * lax.rsqrt(squares + EPS)) * (1.0 / WORKERS)

    diagonal = jnp.where(row == column, gram, 0.0)
    squares = jnp.sum(diagonal, axis=1, keepdims=True)
    squares = jnp.where(squares < jnp.inf, squares, jnp.inf)
    squares_row = jnp.sum(diagonal, axis=0, keepdims=True)
    squares_row = jnp.where(squares_row < jnp.inf, squares_row, jnp.inf)
    first = share(squares)
    first_row = share(squares_row)
    used = jnp.logical_and(column < WORKERS, first_row > 0.0)
    along = jnp.sum(jnp.where(used, first_row * gram, 0.0), axis=1, keepdims=True)
    moved = jnp.sum(jnp.where(first > 0.0, first * along, 0.0), axis=0, keepdims=True)
    again = jnp.maximum(squares - 2.0 * along + moved, 0.0)
    again = jnp.where(squares < jnp.inf, again, jnp.inf)
    second = share(again)
    weight = first * (1.0 - jnp.sum(second, axis=0, keepdims=True)) + second
    bias[...] = jnp.broadcast_to(weight, (WORKERS, LANES))

    def combine(t, carry):
        here = pl.ds(pl.multiple_of(t * 8, 8), 8)
        for q in range(held.shape[2] // LANES):
            there = slice(q * LANES, (q + 1) * LANES)
            sums = [bias[i : i + 1, :] * held[i, here, there] for i in range(WORKERS)]
            while len(sums) > 1:
                sums = [a + b for a, b in zip(sums[::2], sums[1::2], strict=True)]
            out[here, there] = start[here, there] + sums[0]
        return carry

    lax.fori_loop(0, rows // 8, combine, 0)


def solution(mesh):
    def on_device(grads, center, radius):
        grads = grads.reshape(grads.shape[2], grads.shape[3])
        rows, columns = center.shape
        return pl.pallas_call(
            functools.partial(kernel, rows, rows // CHUNKS),
            out_shape=jax.ShapeDtypeStruct((rows, columns), jnp.float32),
            in_specs=[pl.BlockSpec(memory_space=pltpu.HBM), pl.BlockSpec(memory_space=pltpu.HBM), pl.BlockSpec(memory_space=pltpu.SMEM)],
            out_specs=pl.BlockSpec(memory_space=pltpu.VMEM),
            scratch_shapes=[
                pltpu.VMEM((WORKERS, rows, columns), jnp.float32),
                pltpu.VMEM((rows, columns), jnp.float32),
                pltpu.VMEM((WORKERS * WORKERS, 8, LANES), jnp.float32),
                pltpu.VMEM((WORKERS, LANES), jnp.float32),
                pltpu.VMEM((8, LANES), jnp.float32),
                pltpu.VMEM((WORKERS, 8, LANES), jnp.float32),
                pltpu.VMEM((MP + 1, 8, LANES), jnp.float32),
                pltpu.VMEM((WORKERS * WORKERS, LANES), jnp.float32),
                pltpu.SemaphoreType.DMA,
                pltpu.SemaphoreType.DMA((CHUNKS,)),
                pltpu.SemaphoreType.DMA((2,)),
                pltpu.SemaphoreType.DMA((2,)),
                pltpu.SemaphoreType.DMA((2,)),
            ],
            compiler_params=pltpu.CompilerParams(collective_id=0, has_side_effects=True, vmem_limit_bytes=60 * 2**20),
        )(grads, center, radius)

    return jax.shard_map(
        on_device,
        mesh=mesh,
        in_specs=(P("worker", "outer", None, "mp"), P(("worker", "outer"), "mp"), P()),
        out_specs=P(("worker", "outer"), "mp"),
        check_vma=False,
    )
```

```python
import functools
import math

import jax
import jax.numpy as jnp
from jax import lax
from jax.experimental import pallas as pl
from jax.experimental.pallas import tpu as pltpu
from jax.sharding import PartitionSpec as P

MESH = pl.DeviceIdType.MESH
D = 3584
KVW = 4096
WORKERS = 16
EPS = 1e-06
CHUNKS = 14
LANES = 128
BLOCK = 4


def far_chips():
    chips = [(x, y, z) for x in range(4) for y in range(4) for z in range(4) if x or y or z]
    return sorted(chips, key=lambda c: -sum(min(d, 4 - d) for d in c))


def kernel(rows, chunk, grads, center, radius, out, held, start, acc, bias, mine, pair, both, every, lines, sent, landed, near, scalar_sent, scalar_landed, ready):
    w, o, m = lax.axis_index("worker"), lax.axis_index("outer"), lax.axis_index("mp")
    high, core = w // 2, w % 2
    me = w * 4 + o

    own = pltpu.make_async_copy(grads.at[pl.ds(pl.multiple_of(me * rows, 8), rows)], held.at[me], near.at[0])
    base = pltpu.make_async_copy(center, start, near.at[1])
    own.start()
    base.start()

    def device(x, flip, other, y_low=0, z=0):
        column = m // 4
        return ((high + flip) % 2) * 2 + (core + other) % 2, (o + x) % 4, ((column + y_low) % 2) * 4 + (m % 4 + z) % 4

    def greet(semaphore, *offsets):
        pl.semaphore_signal(semaphore, inc=1, device_id=device(*offsets), device_id_type=MESH)

    barrier = pltpu.get_barrier_semaphore()
    first_peers = [(x, 0, c) for x in (2, 1, 3) for c in (0, 1)] + [(0, 1, 0), (0, 1, 1), (0, 0, 1)]
    first_peers += [(0, 0, 0, 0, 1), (0, 0, 0, 0, 3), (0, 0, 0, 1, 0)]
    for offsets in first_peers:
        greet(barrier, *offsets)
    pl.semaphore_wait(barrier, len(first_peers))
    greet(ready.at[0], 0, 1, 0)

    def to(offsets, c):
        worker, outer, part = device(*offsets)
        target = worker * 4 + outer
        at = pl.multiple_of(c * chunk, 8)
        pltpu.make_async_remote_copy(
            src_ref=grads.at[pl.ds(pl.multiple_of(target * rows + at, 8), chunk)],
            dst_ref=held.at[me, pl.ds(at, chunk)],
            send_sem=sent,
            recv_sem=landed.at[c],
            device_id=(worker, outer, part),
            device_id_type=MESH,
        ).start()

    def send(flip, h):
        for x in (1, 3, 2):
            to((x, flip, h % 2), h // 2)

        @pl.when(flip == 0)
        def _():
            to((0, 1, h % 2), h // 2)

    last = 2 * CHUNKS - 1
    send(0, 0)

    @pl.when(core == 0)
    def _():
        send(0, 1)

    pl.semaphore_wait(ready.at[0], 1)

    @pl.when(core == 1)
    def _():
        send(1, 0)

    def turn(s, carry):
        before = s - 1
        send((before + core) % 2, core * (s // 2) + (1 - core) * (before // 2 + 1 - before % 2))
        return carry

    lax.fori_loop(2, 2 * last + 1, turn, 0)
    send(1, last)

    def partner(c, carry):
        to((0, 0, 1), c)
        return carry

    lax.fori_loop(0, CHUNKS, partner, 0)

    greet(ready.at[1], 0, 0, 0, 1, 0)
    pl.semaphore_wait(ready.at[1], 1)
    greet(ready.at[2], 0, 0, 0, 0, 1)
    greet(ready.at[2], 0, 0, 0, 0, 3)
    pl.semaphore_wait(ready.at[2], 2)
    greet(ready.at[3], 0, 0, 0, 0, 3)
    pl.semaphore_wait(ready.at[3], 1)

    acc[...] = jnp.zeros_like(acc)
    own.wait()
    base.wait()

    def gather(c, carry):
        at = pl.multiple_of(c * chunk, 8)
        arrived = held.at[pl.ds(0, WORKERS - 1), pl.ds(at, chunk)]
        pltpu.make_async_copy(arrived, arrived, landed.at[c]).wait()

        def subtract(t, carry):
            here = pl.ds(pl.multiple_of(at + t * 8, 8), 8)
            v = start[here, :]
            for i in range(WORKERS):
                held[i, here, :] = held[i, here, :] - v
            return carry

        lax.fori_loop(0, chunk // 8, subtract, 0)
        for bi in range(WORKERS // BLOCK):
            for bj in range(bi, WORKERS // BLOCK):
                pairs = [(i, j) for i in range(bi * BLOCK, (bi + 1) * BLOCK) for j in range(bj * BLOCK, (bj + 1) * BLOCK) if i <= j]

                def products(t, sums, bi=bi, bj=bj, pairs=pairs):
                    here = pl.ds(pl.multiple_of(at + t * 8, 8), 8)
                    sums = list(sums)
                    for q in range(held.shape[2] // LANES):
                        there = slice(q * LANES, (q + 1) * LANES)
                        d = {i: held[i, here, there] for i in range(bi * BLOCK, (bi + 1) * BLOCK)}
                        for j in range(bj * BLOCK, (bj + 1) * BLOCK):
                            if j not in d:
                                d[j] = held[j, here, there]
                        for k, (i, j) in enumerate(pairs):
                            sums[k] = sums[k] + d[i] * d[j]
                    return tuple(sums)

                sums = lax.fori_loop(0, chunk // 8, products, tuple(acc[i * WORKERS + j] for i, j in pairs))
                for (i, j), total in zip(pairs, sums, strict=True):
                    acc[i * WORKERS + j] = total
        return carry

    lax.fori_loop(0, CHUNKS, gather, 0)

    for i in range(WORKERS):
        at = (i // 8) * LANES + ((8 - i % 8) % 8) * WORKERS
        for j in range(WORKERS):
            lines[at + j : at + j + 1, :] = jnp.sum(acc[min(i, j) * WORKERS + max(i, j)], axis=0, keepdims=True)
    across = lax.dot_general(
        jnp.full((8, LANES), 1.0, jnp.float32),
        lines[...] * 0.0625,
        (((1,), (1,)), ((), ())),
        precision=lax.Precision.HIGHEST,
        preferred_element_type=jnp.float32,
    )
    top = lax.broadcasted_iota(jnp.int32, (8, LANES), 0) == 0
    mine[...] = (jnp.where(top, across[:, :LANES], across[:, LANES:]) * 16.0)[0:2]

    pltpu.make_async_remote_copy(
        src_ref=mine, dst_ref=pair, send_sem=scalar_sent.at[0], recv_sem=scalar_landed.at[0],
        device_id=device(0, 0, 1), device_id_type=MESH,
    ).start()
    pltpu.make_async_copy(pair, pair, scalar_landed.at[0]).wait()
    both[...] = mine[...] + pair[...]
    slot = (o * 4 + high * 2 + m // 4) * 4 + m % 4
    y = high * 2 + m // 4
    for dx, dy, dz in far_chips():
        there = (y + dy) % 4
        pltpu.make_async_remote_copy(
            src_ref=both, dst_ref=every.at[slot], send_sem=scalar_sent.at[1], recv_sem=scalar_landed.at[1],
            device_id=((there // 2) * 2 + core, (o + dx) % 4, (there % 2) * 4 + (m % 4 + dz) % 4), device_id_type=MESH,
        ).start()
    every[slot] = both[...]
    pltpu.make_async_copy(held.at[pl.ds(0, WORKERS - 1)], held.at[pl.ds(0, WORKERS - 1)], sent).wait()
    pltpu.make_async_copy(pair, pair, scalar_sent.at[0]).wait()
    arrived = every.at[pl.ds(0, 63)]
    pltpu.make_async_copy(arrived, arrived, scalar_landed.at[1]).wait()
    pltpu.make_async_copy(arrived, arrived, scalar_sent.at[1]).wait()
    total = jnp.sum(every[...], axis=0)

    tables = [
        pltpu.roll(jnp.broadcast_to(total[h : h + 1, :], (8, LANES)), 0, 1, stride=WORKERS, stride_axis=0) for h in (0, 1)
    ]
    gram = jnp.concatenate(tables, axis=0)
    row = lax.broadcasted_iota(jnp.int32, (WORKERS, LANES), 0)
    column = lax.broadcasted_iota(jnp.int32, (WORKERS, LANES), 1)
    tau = radius[0] * math.sqrt(D * KVW)

    def share(squares):
        return jnp.minimum(1.0, tau * lax.rsqrt(squares + EPS)) * (1.0 / WORKERS)

    diagonal = jnp.where(row == column, gram, 0.0)
    squares = jnp.sum(diagonal, axis=1, keepdims=True)
    squares = jnp.where(squares < jnp.inf, squares, jnp.inf)
    squares_row = jnp.sum(diagonal, axis=0, keepdims=True)
    squares_row = jnp.where(squares_row < jnp.inf, squares_row, jnp.inf)
    first = share(squares)
    first_row = share(squares_row)
    used = jnp.logical_and(column < WORKERS, first_row > 0.0)
    along = jnp.sum(jnp.where(used, first_row * gram, 0.0), axis=1, keepdims=True)
    moved = jnp.sum(jnp.where(first > 0.0, first * along, 0.0), axis=0, keepdims=True)
    again = jnp.maximum(squares - 2.0 * along + moved, 0.0)
    again = jnp.where(squares < jnp.inf, again, jnp.inf)
    second = share(again)
    weight = first * (1.0 - jnp.sum(second, axis=0, keepdims=True)) + second
    bias[...] = jnp.broadcast_to(weight, (WORKERS, LANES))

    def combine(t, carry):
        here = pl.ds(pl.multiple_of(t * 8, 8), 8)
        for q in range(held.shape[2] // LANES):
            there = slice(q * LANES, (q + 1) * LANES)
            sums = [bias[i : i + 1, :] * held[i, here, there] for i in range(WORKERS)]
            while len(sums) > 1:
                sums = [a + b for a, b in zip(sums[::2], sums[1::2], strict=True)]
            out[here, there] = start[here, there] + sums[0]
        return carry

    lax.fori_loop(0, rows // 8, combine, 0)


def solution(mesh):
    def on_device(grads, center, radius):
        grads = grads.reshape(grads.shape[2], grads.shape[3])
        rows, columns = center.shape
        return pl.pallas_call(
            functools.partial(kernel, rows, rows // CHUNKS),
            out_shape=pltpu.VMEM((rows, columns), jnp.float32),
            in_specs=[pl.BlockSpec(memory_space=pltpu.HBM), pl.BlockSpec(memory_space=pltpu.HBM), pl.BlockSpec(memory_space=pltpu.SMEM)],
            out_specs=pl.BlockSpec(memory_space=pltpu.VMEM),
            scratch_shapes=[
                pltpu.VMEM((WORKERS, rows, columns), jnp.float32),
                pltpu.VMEM((rows, columns), jnp.float32),
                pltpu.VMEM((WORKERS * WORKERS, 8, LANES), jnp.float32),
                pltpu.VMEM((WORKERS, LANES), jnp.float32),
                pltpu.VMEM((2, LANES), jnp.float32),
                pltpu.VMEM((2, LANES), jnp.float32),
                pltpu.VMEM((2, LANES), jnp.float32),
                pltpu.VMEM((64, 2, LANES), jnp.float32),
                pltpu.VMEM((WORKERS * WORKERS, LANES), jnp.float32),
                pltpu.SemaphoreType.DMA,
                pltpu.SemaphoreType.DMA((CHUNKS,)),
                pltpu.SemaphoreType.DMA((2,)),
                pltpu.SemaphoreType.DMA((2,)),
                pltpu.SemaphoreType.DMA((2,)),
                pltpu.SemaphoreType.REGULAR((4,)),
            ],
            compiler_params=pltpu.CompilerParams(collective_id=0, has_side_effects=True, vmem_limit_bytes=60 * 2**20),
        )(grads, center, radius)

    return jax.shard_map(
        on_device,
        mesh=mesh,
        in_specs=(P("worker", "outer", None, "mp"), P(("worker", "outer"), "mp"), P()),
        out_specs=P(("worker", "outer"), "mp"),
        check_vma=False,
    )
```

```python
import functools
import math

import jax
import jax.numpy as jnp
from jax import lax
from jax.experimental import pallas as pl
from jax.experimental.pallas import tpu as pltpu
from jax.sharding import PartitionSpec as P

MESH = pl.DeviceIdType.MESH
D = 3584
KVW = 4096
WORKERS = 16
EPS = 1e-06
CHUNKS = 14
LANES = 128
BLOCK = 4


def far_chips():
    chips = [(x, y, z) for x in range(4) for y in range(4) for z in range(4) if x or y or z]
    return sorted(chips, key=lambda c: -sum(min(d, 4 - d) for d in c))


def kernel(rows, chunk, grads, center, radius, out, held, start, acc, bias, mine, pair, both, every, lines, sent, landed, near, scalar_sent, scalar_landed, ready):
    w, o, m = lax.axis_index("worker"), lax.axis_index("outer"), lax.axis_index("mp")
    high, core = w // 2, w % 2
    me = w * 4 + o

    own = pltpu.make_async_copy(grads.at[pl.ds(pl.multiple_of(me * rows, 8), rows)], held.at[me], near.at[0])
    base = pltpu.make_async_copy(center, start, near.at[1])
    own.start()
    base.start()

    def device(x, flip, other, y_low=0, z=0):
        column = m // 4
        return ((high + flip) % 2) * 2 + (core + other) % 2, (o + x) % 4, ((column + y_low) % 2) * 4 + (m % 4 + z) % 4

    def greet(semaphore, *offsets):
        pl.semaphore_signal(semaphore, inc=1, device_id=device(*offsets), device_id_type=MESH)

    barrier = pltpu.get_barrier_semaphore()
    nearest = [(2, 0, 0), (0, 1, 0), (1, 0, 0), (3, 0, 0), (0, 0, 0, 0, 1), (0, 0, 0, 0, 3), (0, 0, 0, 1, 0), (0, 0, 1)]
    for offsets in nearest:
        greet(barrier, *offsets)
    pl.semaphore_wait(barrier, len(nearest))
    greet(ready.at[0], 0, 0, 1)
    greet(ready.at[1], 0, 1, 0)

    def to(offsets, c):
        worker, outer, part = device(*offsets)
        target = worker * 4 + outer
        at = pl.multiple_of(c * chunk, 8)
        pltpu.make_async_remote_copy(
            src_ref=grads.at[pl.ds(pl.multiple_of(target * rows + at, 8), chunk)],
            dst_ref=held.at[me, pl.ds(at, chunk)],
            send_sem=sent,
            recv_sem=landed.at[c],
            device_id=(worker, outer, part),
            device_id_type=MESH,
        ).start()

    def send(flip, h):
        for x in (1, 3, 2):
            to((x, flip, h % 2), h // 2)

        @pl.when(flip == 0)
        def _():
            to((0, 1, h % 2), h // 2)

    last = 2 * CHUNKS - 1
    send(0, 0)
    pl.semaphore_wait(ready.at[0], 1)

    @pl.when(core == 0)
    def _():
        send(0, 1)

    pl.semaphore_wait(ready.at[1], 1)
    greet(ready.at[2], 0, 0, 1)

    @pl.when(core == 1)
    def _():
        send(1, 0)

    pl.semaphore_wait(ready.at[2], 1)

    def partner(c, carry):
        to((0, 0, 1), c)
        return carry

    lax.fori_loop(0, CHUNKS, partner, 0)

    def turn(s, carry):
        before = s - 1
        send((before + core) % 2, core * (s // 2) + (1 - core) * (before // 2 + 1 - before % 2))
        return carry

    lax.fori_loop(2, 2 * last - 1, turn, 0)
    send(1, last - 1)
    send(1, last)
    send(0, last)

    greet(ready.at[3], 0, 0, 0, 1, 0)
    pl.semaphore_wait(ready.at[3], 1)
    greet(ready.at[4], 0, 0, 0, 0, 1)
    greet(ready.at[4], 0, 0, 0, 0, 3)
    pl.semaphore_wait(ready.at[4], 2)
    greet(ready.at[5], 0, 0, 0, 0, 3)
    pl.semaphore_wait(ready.at[5], 1)

    acc[...] = jnp.zeros_like(acc)
    own.wait()
    base.wait()

    def gather(c, carry):
        at = pl.multiple_of(c * chunk, 8)
        arrived = held.at[pl.ds(0, WORKERS - 1), pl.ds(at, chunk)]
        pltpu.make_async_copy(arrived, arrived, landed.at[c]).wait()

        def subtract(t, carry):
            here = pl.ds(pl.multiple_of(at + t * 8, 8), 8)
            v = start[here, :]
            for i in range(WORKERS):
                held[i, here, :] = held[i, here, :] - v
            return carry

        lax.fori_loop(0, chunk // 8, subtract, 0)
        for bi in range(WORKERS // BLOCK):
            for bj in range(bi, WORKERS // BLOCK):
                pairs = [(i, j) for i in range(bi * BLOCK, (bi + 1) * BLOCK) for j in range(bj * BLOCK, (bj + 1) * BLOCK) if i <= j]

                def products(t, sums, bi=bi, bj=bj, pairs=pairs):
                    here = pl.ds(pl.multiple_of(at + t * 8, 8), 8)
                    sums = list(sums)
                    for q in range(held.shape[2] // LANES):
                        there = slice(q * LANES, (q + 1) * LANES)
                        d = {i: held[i, here, there] for i in range(bi * BLOCK, (bi + 1) * BLOCK)}
                        for j in range(bj * BLOCK, (bj + 1) * BLOCK):
                            if j not in d:
                                d[j] = held[j, here, there]
                        for k, (i, j) in enumerate(pairs):
                            sums[k] = sums[k] + d[i] * d[j]
                    return tuple(sums)

                sums = lax.fori_loop(0, chunk // 8, products, tuple(acc[i * WORKERS + j] for i, j in pairs))
                for (i, j), total in zip(pairs, sums, strict=True):
                    acc[i * WORKERS + j] = total
        return carry

    lax.fori_loop(0, CHUNKS, gather, 0)

    for i in range(WORKERS):
        at = (i // 8) * LANES + ((8 - i % 8) % 8) * WORKERS
        for j in range(WORKERS):
            lines[at + j : at + j + 1, :] = jnp.sum(acc[min(i, j) * WORKERS + max(i, j)], axis=0, keepdims=True)
    across = lax.dot_general(
        jnp.full((8, LANES), 1.0, jnp.float32),
        lines[...] * 0.0625,
        (((1,), (1,)), ((), ())),
        precision=lax.Precision.HIGHEST,
        preferred_element_type=jnp.float32,
    )
    top = lax.broadcasted_iota(jnp.int32, (8, LANES), 0) == 0
    mine[...] = (jnp.where(top, across[:, :LANES], across[:, LANES:]) * 16.0)[0:2]

    pltpu.make_async_remote_copy(
        src_ref=mine, dst_ref=pair, send_sem=scalar_sent.at[0], recv_sem=scalar_landed.at[0],
        device_id=device(0, 0, 1), device_id_type=MESH,
    ).start()
    pltpu.make_async_copy(pair, pair, scalar_landed.at[0]).wait()
    both[...] = mine[...] + pair[...]
    slot = (o * 4 + high * 2 + m // 4) * 4 + m % 4
    y = high * 2 + m // 4
    for dx, dy, dz in far_chips():
        there = (y + dy) % 4
        pltpu.make_async_remote_copy(
            src_ref=both, dst_ref=every.at[slot], send_sem=scalar_sent.at[1], recv_sem=scalar_landed.at[1],
            device_id=((there // 2) * 2 + core, (o + dx) % 4, (there % 2) * 4 + (m % 4 + dz) % 4), device_id_type=MESH,
        ).start()
    every[slot] = both[...]
    pltpu.make_async_copy(held.at[pl.ds(0, WORKERS - 1)], held.at[pl.ds(0, WORKERS - 1)], sent).wait()
    pltpu.make_async_copy(pair, pair, scalar_sent.at[0]).wait()
    arrived = every.at[pl.ds(0, 63)]
    pltpu.make_async_copy(arrived, arrived, scalar_landed.at[1]).wait()
    pltpu.make_async_copy(arrived, arrived, scalar_sent.at[1]).wait()
    total = jnp.sum(every[...], axis=0)

    tables = [
        pltpu.roll(jnp.broadcast_to(total[h : h + 1, :], (8, LANES)), 0, 1, stride=WORKERS, stride_axis=0) for h in (0, 1)
    ]
    gram = jnp.concatenate(tables, axis=0)
    row = lax.broadcasted_iota(jnp.int32, (WORKERS, LANES), 0)
    column = lax.broadcasted_iota(jnp.int32, (WORKERS, LANES), 1)
    tau = radius[0] * math.sqrt(D * KVW)

    def share(squares):
        return jnp.minimum(1.0, tau * lax.rsqrt(squares + EPS)) * (1.0 / WORKERS)

    diagonal = jnp.where(row == column, gram, 0.0)
    squares = jnp.sum(diagonal, axis=1, keepdims=True)
    squares = jnp.where(squares < jnp.inf, squares, jnp.inf)
    squares_row = jnp.sum(diagonal, axis=0, keepdims=True)
    squares_row = jnp.where(squares_row < jnp.inf, squares_row, jnp.inf)
    first = share(squares)
    first_row = share(squares_row)
    used = jnp.logical_and(column < WORKERS, first_row > 0.0)
    along = jnp.sum(jnp.where(used, first_row * gram, 0.0), axis=1, keepdims=True)
    moved = jnp.sum(jnp.where(first > 0.0, first * along, 0.0), axis=0, keepdims=True)
    again = jnp.maximum(squares - 2.0 * along + moved, 0.0)
    again = jnp.where(squares < jnp.inf, again, jnp.inf)
    second = share(again)
    weight = first * (1.0 - jnp.sum(second, axis=0, keepdims=True)) + second
    bias[...] = jnp.broadcast_to(weight, (WORKERS, LANES))

    def combine(t, carry):
        here = pl.ds(pl.multiple_of(t * 8, 8), 8)
        for q in range(held.shape[2] // LANES):
            there = slice(q * LANES, (q + 1) * LANES)
            sums = [bias[i : i + 1, :] * held[i, here, there] for i in range(WORKERS)]
            while len(sums) > 1:
                sums = [a + b for a, b in zip(sums[::2], sums[1::2], strict=True)]
            out[here, there] = start[here, there] + sums[0]
        return carry

    lax.fori_loop(0, rows // 8, combine, 0)


def solution(mesh):
    def on_device(grads, center, radius):
        grads = grads.reshape(grads.shape[2], grads.shape[3])
        rows, columns = center.shape
        return pl.pallas_call(
            functools.partial(kernel, rows, rows // CHUNKS),
            out_shape=pltpu.VMEM((rows, columns), jnp.float32),
            in_specs=[pl.BlockSpec(memory_space=pltpu.HBM), pl.BlockSpec(memory_space=pltpu.HBM), pl.BlockSpec(memory_space=pltpu.SMEM)],
            out_specs=pl.BlockSpec(memory_space=pltpu.VMEM),
            scratch_shapes=[
                pltpu.VMEM((WORKERS, rows, columns), jnp.float32),
                pltpu.VMEM((rows, columns), jnp.float32),
                pltpu.VMEM((WORKERS * WORKERS, 8, LANES), jnp.float32),
                pltpu.VMEM((WORKERS, LANES), jnp.float32),
                pltpu.VMEM((2, LANES), jnp.float32),
                pltpu.VMEM((2, LANES), jnp.float32),
                pltpu.VMEM((2, LANES), jnp.float32),
                pltpu.VMEM((64, 2, LANES), jnp.float32),
                pltpu.VMEM((WORKERS * WORKERS, LANES), jnp.float32),
                pltpu.SemaphoreType.DMA,
                pltpu.SemaphoreType.DMA((CHUNKS,)),
                pltpu.SemaphoreType.DMA((2,)),
                pltpu.SemaphoreType.DMA((2,)),
                pltpu.SemaphoreType.DMA((2,)),
                pltpu.SemaphoreType.REGULAR((6,)),
            ],
            compiler_params=pltpu.CompilerParams(collective_id=0, has_side_effects=True, vmem_limit_bytes=60 * 2**20),
        )(grads, center, radius)

    return jax.shard_map(
        on_device,
        mesh=mesh,
        in_specs=(P("worker", "outer", None, "mp"), P(("worker", "outer"), "mp"), P()),
        out_specs=P(("worker", "outer"), "mp"),
        check_vma=False,
    )
```

```python
import functools
import math

import jax
import jax.numpy as jnp
from jax import lax
from jax.experimental import pallas as pl
from jax.experimental.pallas import tpu as pltpu
from jax.sharding import PartitionSpec as P

MESH = pl.DeviceIdType.MESH
D = 3584
KVW = 4096
WORKERS = 16
EPS = 1e-06
CHUNKS = 14
LANES = 128
BLOCK = 4


def far_devices():
    devices = [(x, y, z, c) for c in (0, 1) for x in range(4) for y in range(4) for z in range(4) if x or y or z or c]
    return sorted(devices, key=lambda d: -sum(min(k, 4 - k) for k in d[:3]))


def kernel(rows, chunk, grads, center, radius, out, held, start, acc, bias, mine, every, lines, sent, landed, near, scalar_sent, scalar_landed, ready):
    w, o, m = lax.axis_index("worker"), lax.axis_index("outer"), lax.axis_index("mp")
    high, core = w // 2, w % 2
    me = w * 4 + o

    own = pltpu.make_async_copy(grads.at[pl.ds(pl.multiple_of(me * rows, 8), rows)], held.at[me], near.at[0])
    base = pltpu.make_async_copy(center, start, near.at[1])
    own.start()
    base.start()

    def device(x, flip, other, y_low=0, z=0):
        column = m // 4
        return ((high + flip) % 2) * 2 + (core + other) % 2, (o + x) % 4, ((column + y_low) % 2) * 4 + (m % 4 + z) % 4

    def greet(semaphore, *offsets):
        pl.semaphore_signal(semaphore, inc=1, device_id=device(*offsets), device_id_type=MESH)

    barrier = pltpu.get_barrier_semaphore()
    nearest = [(2, 0, 0), (0, 1, 0), (1, 0, 0), (3, 0, 0), (0, 0, 0, 0, 1), (0, 0, 0, 0, 3), (0, 0, 0, 1, 0), (0, 0, 1)]
    for offsets in nearest:
        greet(barrier, *offsets)
    pl.semaphore_wait(barrier, len(nearest))
    greet(ready.at[0], 0, 0, 1)
    greet(ready.at[1], 0, 1, 0)

    def to(offsets, c):
        worker, outer, part = device(*offsets)
        target = worker * 4 + outer
        at = pl.multiple_of(c * chunk, 8)
        pltpu.make_async_remote_copy(
            src_ref=grads.at[pl.ds(pl.multiple_of(target * rows + at, 8), chunk)],
            dst_ref=held.at[me, pl.ds(at, chunk)],
            send_sem=sent,
            recv_sem=landed.at[c],
            device_id=(worker, outer, part),
            device_id_type=MESH,
        ).start()

    def send(flip, h):
        for x in (1, 3, 2):
            to((x, flip, h % 2), h // 2)

        @pl.when(flip == 0)
        def _():
            to((0, 1, h % 2), h // 2)

    last = 2 * CHUNKS - 1
    send(0, 0)
    pl.semaphore_wait(ready.at[0], 1)

    @pl.when(core == 0)
    def _():
        send(0, 1)

    pl.semaphore_wait(ready.at[1], 1)
    greet(ready.at[2], 0, 0, 1)

    @pl.when(core == 1)
    def _():
        send(1, 0)

    pl.semaphore_wait(ready.at[2], 1)

    def partner(c, carry):
        to((0, 0, 1), c)
        return carry

    lax.fori_loop(0, CHUNKS, partner, 0)

    def turn(s, carry):
        before = s - 1
        send((before + core) % 2, core * (s // 2) + (1 - core) * (before // 2 + 1 - before % 2))
        return carry

    lax.fori_loop(2, 2 * last - 1, turn, 0)
    send(1, last - 1)
    send(1, last)
    send(0, last)

    greet(ready.at[3], 0, 0, 0, 1, 0)
    pl.semaphore_wait(ready.at[3], 1)
    greet(ready.at[4], 0, 0, 0, 0, 1)
    greet(ready.at[4], 0, 0, 0, 0, 3)
    pl.semaphore_wait(ready.at[4], 2)
    greet(ready.at[5], 0, 0, 0, 0, 3)
    pl.semaphore_wait(ready.at[5], 1)

    acc[...] = jnp.zeros_like(acc)
    own.wait()
    base.wait()

    def gather(c, carry):
        at = pl.multiple_of(c * chunk, 8)
        arrived = held.at[pl.ds(0, WORKERS - 1), pl.ds(at, chunk)]
        pltpu.make_async_copy(arrived, arrived, landed.at[c]).wait()

        def subtract(t, carry):
            here = pl.ds(pl.multiple_of(at + t * 8, 8), 8)
            v = start[here, :]
            for i in range(WORKERS):
                held[i, here, :] = held[i, here, :] - v
            return carry

        lax.fori_loop(0, chunk // 8, subtract, 0)
        for bi in range(WORKERS // BLOCK):
            for bj in range(bi, WORKERS // BLOCK):
                pairs = [(i, j) for i in range(bi * BLOCK, (bi + 1) * BLOCK) for j in range(bj * BLOCK, (bj + 1) * BLOCK) if i <= j]

                def products(t, sums, bi=bi, bj=bj, pairs=pairs):
                    here = pl.ds(pl.multiple_of(at + t * 8, 8), 8)
                    sums = list(sums)
                    for q in range(held.shape[2] // LANES):
                        there = slice(q * LANES, (q + 1) * LANES)
                        d = {i: held[i, here, there] for i in range(bi * BLOCK, (bi + 1) * BLOCK)}
                        for j in range(bj * BLOCK, (bj + 1) * BLOCK):
                            if j not in d:
                                d[j] = held[j, here, there]
                        for k, (i, j) in enumerate(pairs):
                            sums[k] = sums[k] + d[i] * d[j]
                    return tuple(sums)

                sums = lax.fori_loop(0, chunk // 8, products, tuple(acc[i * WORKERS + j] for i, j in pairs))
                for (i, j), total in zip(pairs, sums, strict=True):
                    acc[i * WORKERS + j] = total
        return carry

    lax.fori_loop(0, CHUNKS, gather, 0)

    def line(i, j):
        return (i // 8) * LANES + ((8 - i % 8) % 8) * WORKERS + j

    for i in range(WORKERS):
        for j in range(i, WORKERS):
            whole = jnp.sum(acc[i * WORKERS + j], axis=0, keepdims=True)
            for at in sorted({line(i, j), line(j, i)}):
                lines[at : at + 1, :] = whole
    across = lax.dot_general(
        jnp.full((8, LANES), 1.0, jnp.float32),
        lines[...] * 0.0625,
        (((1,), (1,)), ((), ())),
        precision=lax.Precision.HIGHEST,
        preferred_element_type=jnp.float32,
    )
    top = lax.broadcasted_iota(jnp.int32, (8, LANES), 0) == 0
    mine[...] = (jnp.where(top, across[:, :LANES], across[:, LANES:]) * 16.0)[0:2]

    y = high * 2 + m // 4
    slot = ((o * 4 + y) * 4 + m % 4) * 2 + core
    for dx, dy, dz, dc in far_devices():
        there = (y + dy) % 4
        pltpu.make_async_remote_copy(
            src_ref=mine, dst_ref=every.at[slot], send_sem=scalar_sent, recv_sem=scalar_landed,
            device_id=((there // 2) * 2 + (core + dc) % 2, (o + dx) % 4, (there % 2) * 4 + (m % 4 + dz) % 4),
            device_id_type=MESH,
        ).start()
    every[slot] = mine[...]
    pltpu.make_async_copy(held.at[pl.ds(0, WORKERS - 1)], held.at[pl.ds(0, WORKERS - 1)], sent).wait()
    arrived = every.at[pl.ds(0, 127)]
    pltpu.make_async_copy(arrived, arrived, scalar_landed).wait()
    total = jnp.sum(every[...], axis=0)

    tables = [
        pltpu.roll(jnp.broadcast_to(total[h : h + 1, :], (8, LANES)), 0, 1, stride=WORKERS, stride_axis=0) for h in (0, 1)
    ]
    gram = jnp.concatenate(tables, axis=0)
    row = lax.broadcasted_iota(jnp.int32, (WORKERS, LANES), 0)
    column = lax.broadcasted_iota(jnp.int32, (WORKERS, LANES), 1)
    tau = radius[0] * math.sqrt(D * KVW)

    def share(squares):
        return jnp.minimum(1.0, tau * lax.rsqrt(squares + EPS)) * (1.0 / WORKERS)

    diagonal = jnp.where(row == column, gram, 0.0)
    squares = jnp.sum(diagonal, axis=1, keepdims=True)
    squares = jnp.where(squares < jnp.inf, squares, jnp.inf)
    squares_row = jnp.sum(diagonal, axis=0, keepdims=True)
    squares_row = jnp.where(squares_row < jnp.inf, squares_row, jnp.inf)
    first = share(squares)
    first_row = share(squares_row)
    used = jnp.logical_and(column < WORKERS, first_row > 0.0)
    along = jnp.sum(jnp.where(used, first_row * gram, 0.0), axis=1, keepdims=True)
    moved = jnp.sum(jnp.where(first > 0.0, first * along, 0.0), axis=0, keepdims=True)
    again = jnp.maximum(squares - 2.0 * along + moved, 0.0)
    again = jnp.where(squares < jnp.inf, again, jnp.inf)
    second = share(again)
    weight = first * (1.0 - jnp.sum(second, axis=0, keepdims=True)) + second
    bias[...] = jnp.broadcast_to(weight, (WORKERS, LANES))

    weights = [jnp.broadcast_to(bias[i : i + 1, :], (8, LANES)) for i in range(WORKERS)]

    def combine(t, carry):
        here = pl.ds(pl.multiple_of(t * 8, 8), 8)
        for q in range(held.shape[2] // LANES):
            there = slice(q * LANES, (q + 1) * LANES)
            sums = [weights[i] * held[i, here, there] for i in range(WORKERS)]
            while len(sums) > 1:
                sums = [a + b for a, b in zip(sums[::2], sums[1::2], strict=True)]
            out[here, there] = start[here, there] + sums[0]
        return carry

    lax.fori_loop(0, rows // 8, combine, 0, unroll=2)
    pltpu.make_async_copy(arrived, arrived, scalar_sent).wait()


def solution(mesh):
    def on_device(grads, center, radius):
        grads = grads.reshape(grads.shape[2], grads.shape[3])
        rows, columns = center.shape
        return pl.pallas_call(
            functools.partial(kernel, rows, rows // CHUNKS),
            out_shape=pltpu.VMEM((rows, columns), jnp.float32),
            in_specs=[pl.BlockSpec(memory_space=pltpu.HBM), pl.BlockSpec(memory_space=pltpu.HBM), pl.BlockSpec(memory_space=pltpu.SMEM)],
            out_specs=pl.BlockSpec(memory_space=pltpu.VMEM),
            scratch_shapes=[
                pltpu.VMEM((WORKERS, rows, columns), jnp.float32),
                pltpu.VMEM((rows, columns), jnp.float32),
                pltpu.VMEM((WORKERS * WORKERS, 8, LANES), jnp.float32),
                pltpu.VMEM((WORKERS, LANES), jnp.float32),
                pltpu.VMEM((2, LANES), jnp.float32),
                pltpu.VMEM((128, 2, LANES), jnp.float32),
                pltpu.VMEM((WORKERS * WORKERS, LANES), jnp.float32),
                pltpu.SemaphoreType.DMA,
                pltpu.SemaphoreType.DMA((CHUNKS,)),
                pltpu.SemaphoreType.DMA((2,)),
                pltpu.SemaphoreType.DMA,
                pltpu.SemaphoreType.DMA,
                pltpu.SemaphoreType.REGULAR((6,)),
            ],
            compiler_params=pltpu.CompilerParams(collective_id=0, has_side_effects=True, vmem_limit_bytes=60 * 2**20),
        )(grads, center, radius)

    return jax.shard_map(
        on_device,
        mesh=mesh,
        in_specs=(P("worker", "outer", None, "mp"), P(("worker", "outer"), "mp"), P()),
        out_specs=P(("worker", "outer"), "mp"),
        check_vma=False,
    )
```

```python
import functools
import math

import jax
import jax.numpy as jnp
from jax import lax
from jax.experimental import pallas as pl
from jax.experimental.pallas import tpu as pltpu
from jax.sharding import PartitionSpec as P

MESH = pl.DeviceIdType.MESH
D = 3584
KVW = 4096
WORKERS = 16
EPS = 1e-06
CHUNKS = 14
LANES = 128
BLOCK = 4


def far_devices():
    devices = [(x, y, z, c) for c in (0, 1) for x in range(4) for y in range(4) for z in range(4) if x or y or z or c]
    return sorted(devices, key=lambda d: (-sum(min(k, 4 - k) for k in d[:3]), -min(d[2], 4 - d[2])))


def kernel(rows, chunk, grads, center, radius, out, held, start, acc, bias, mine, every, lines, sent, landed, near, scalar_sent, scalar_landed, ready):
    w, o, m = lax.axis_index("worker"), lax.axis_index("outer"), lax.axis_index("mp")
    high, core = w // 2, w % 2
    me = w * 4 + o

    own = pltpu.make_async_copy(grads.at[pl.ds(pl.multiple_of(me * rows, 8), rows)], held.at[me], near.at[0])
    base = pltpu.make_async_copy(center, start, near.at[1])
    own.start()
    base.start()

    def device(x, flip, other, y_low=0, z=0):
        column = m // 4
        return ((high + flip) % 2) * 2 + (core + other) % 2, (o + x) % 4, ((column + y_low) % 2) * 4 + (m % 4 + z) % 4

    def greet(semaphore, *offsets):
        pl.semaphore_signal(semaphore, inc=1, device_id=device(*offsets), device_id_type=MESH)

    barrier = pltpu.get_barrier_semaphore()
    nearest = [(2, 0, 0), (0, 1, 0), (1, 0, 0), (3, 0, 0), (0, 0, 0, 0, 1), (0, 0, 0, 0, 3), (0, 0, 0, 1, 0), (0, 0, 1)]
    for offsets in nearest:
        greet(barrier, *offsets)
    pl.semaphore_wait(barrier, len(nearest))
    greet(ready.at[0], 0, 0, 1)
    greet(ready.at[1], 0, 1, 0)

    def to(offsets, c):
        worker, outer, part = device(*offsets)
        target = worker * 4 + outer
        at = pl.multiple_of(c * chunk, 8)
        pltpu.make_async_remote_copy(
            src_ref=grads.at[pl.ds(pl.multiple_of(target * rows + at, 8), chunk)],
            dst_ref=held.at[me, pl.ds(at, chunk)],
            send_sem=sent,
            recv_sem=landed.at[c],
            device_id=(worker, outer, part),
            device_id_type=MESH,
        ).start()

    def send(flip, h):
        for x in (1, 3, 2):
            to((x, flip, h % 2), h // 2)

        @pl.when(flip == 0)
        def _():
            to((0, 1, h % 2), h // 2)

    last = 2 * CHUNKS - 1
    send(0, 0)
    pl.semaphore_wait(ready.at[0], 1)

    @pl.when(core == 0)
    def _():
        send(0, 1)

    pl.semaphore_wait(ready.at[1], 1)
    greet(ready.at[2], 0, 0, 1)

    @pl.when(core == 1)
    def _():
        send(1, 0)

    pl.semaphore_wait(ready.at[2], 1)

    def partner(c, carry):
        to((0, 0, 1), c)
        return carry

    lax.fori_loop(0, CHUNKS, partner, 0)

    def turn(s, carry):
        before = s - 1
        send((before + core) % 2, core * (s // 2) + (1 - core) * (before // 2 + 1 - before % 2))
        return carry

    lax.fori_loop(2, 2 * last - 1, turn, 0)
    send(1, last - 1)
    send(1, last)
    send(0, last)

    greet(ready.at[3], 0, 0, 0, 1, 0)
    pl.semaphore_wait(ready.at[3], 1)
    greet(ready.at[4], 0, 0, 0, 0, 1)
    greet(ready.at[4], 0, 0, 0, 0, 3)
    pl.semaphore_wait(ready.at[4], 2)
    greet(ready.at[5], 0, 0, 0, 0, 3)
    pl.semaphore_wait(ready.at[5], 1)

    acc[...] = jnp.zeros_like(acc)
    own.wait()
    base.wait()

    def gather(c, carry):
        at = pl.multiple_of(c * chunk, 8)
        arrived = held.at[pl.ds(0, WORKERS - 1), pl.ds(at, chunk)]
        pltpu.make_async_copy(arrived, arrived, landed.at[c]).wait()

        def subtract(t, carry):
            here = pl.ds(pl.multiple_of(at + t * 8, 8), 8)
            v = start[here, :]
            for i in range(WORKERS):
                held[i, here, :] = held[i, here, :] - v
            return carry

        lax.fori_loop(0, chunk // 8, subtract, 0)
        for bi in range(WORKERS // BLOCK):
            for bj in range(bi, WORKERS // BLOCK):
                pairs = [(i, j) for i in range(bi * BLOCK, (bi + 1) * BLOCK) for j in range(bj * BLOCK, (bj + 1) * BLOCK) if i <= j]

                def products(t, sums, bi=bi, bj=bj, pairs=pairs):
                    here = pl.ds(pl.multiple_of(at + t * 8, 8), 8)
                    sums = list(sums)
                    for q in range(held.shape[2] // LANES):
                        there = slice(q * LANES, (q + 1) * LANES)
                        d = {i: held[i, here, there] for i in range(bi * BLOCK, (bi + 1) * BLOCK)}
                        for j in range(bj * BLOCK, (bj + 1) * BLOCK):
                            if j not in d:
                                d[j] = held[j, here, there]
                        for k, (i, j) in enumerate(pairs):
                            sums[k] = sums[k] + d[i] * d[j]
                    return tuple(sums)

                sums = lax.fori_loop(0, chunk // 8, products, tuple(acc[i * WORKERS + j] for i, j in pairs))
                for (i, j), total in zip(pairs, sums, strict=True):
                    acc[i * WORKERS + j] = total
        return carry

    lax.fori_loop(0, CHUNKS, gather, 0)

    def line(i, j):
        return (i // 8) * LANES + ((8 - i % 8) % 8) * WORKERS + j

    for i in range(WORKERS):
        for j in range(i, WORKERS):
            whole = jnp.sum(acc[i * WORKERS + j], axis=0, keepdims=True)
            for at in sorted({line(i, j), line(j, i)}):
                lines[at : at + 1, :] = whole
    across = lax.dot_general(
        jnp.full((8, LANES), 1.0, jnp.float32),
        lines[...] * 0.0625,
        (((1,), (1,)), ((), ())),
        precision=lax.Precision.HIGHEST,
        preferred_element_type=jnp.float32,
    )
    top = lax.broadcasted_iota(jnp.int32, (8, LANES), 0) == 0
    mine[...] = (jnp.where(top, across[:, :LANES], across[:, LANES:]) * 16.0)[0:2]

    y = high * 2 + m // 4
    slot = ((o * 4 + y) * 4 + m % 4) * 2 + core
    for dx, dy, dz, dc in far_devices():
        there = (y + dy) % 4
        pltpu.make_async_remote_copy(
            src_ref=mine, dst_ref=every.at[slot], send_sem=scalar_sent, recv_sem=scalar_landed,
            device_id=((there // 2) * 2 + (core + dc) % 2, (o + dx) % 4, (there % 2) * 4 + (m % 4 + dz) % 4),
            device_id_type=MESH,
        ).start()
    every[slot] = mine[...]
    pltpu.make_async_copy(held.at[pl.ds(0, WORKERS - 1)], held.at[pl.ds(0, WORKERS - 1)], sent).wait()
    arrived = every.at[pl.ds(0, 127)]
    pltpu.make_async_copy(arrived, arrived, scalar_landed).wait()
    total = jnp.sum(jnp.sum(every[...].reshape(16, 8, 2, LANES), axis=0), axis=0)

    tables = [
        pltpu.roll(jnp.broadcast_to(total[h : h + 1, :], (8, LANES)), 0, 1, stride=WORKERS, stride_axis=0) for h in (0, 1)
    ]
    gram = jnp.concatenate(tables, axis=0)
    row = lax.broadcasted_iota(jnp.int32, (WORKERS, LANES), 0)
    column = lax.broadcasted_iota(jnp.int32, (WORKERS, LANES), 1)
    tau = radius[0] * math.sqrt(D * KVW)

    def share(squares):
        return jnp.minimum(1.0, tau * lax.rsqrt(squares + EPS)) * (1.0 / WORKERS)

    diagonal = jnp.where(row == column, gram, 0.0)
    squares = jnp.sum(diagonal, axis=1, keepdims=True)
    squares = jnp.where(squares < jnp.inf, squares, jnp.inf)
    squares_row = jnp.sum(diagonal, axis=0, keepdims=True)
    squares_row = jnp.where(squares_row < jnp.inf, squares_row, jnp.inf)
    first = share(squares)
    first_row = share(squares_row)
    used = jnp.logical_and(column < WORKERS, first_row > 0.0)
    along = jnp.sum(jnp.where(used, first_row * gram, 0.0), axis=1, keepdims=True)
    moved = jnp.sum(jnp.where(first > 0.0, first * along, 0.0), axis=0, keepdims=True)
    again = jnp.maximum(squares - 2.0 * along + moved, 0.0)
    again = jnp.where(squares < jnp.inf, again, jnp.inf)
    second = share(again)
    weight = first * (1.0 - jnp.sum(second, axis=0, keepdims=True)) + second
    bias[...] = jnp.broadcast_to(weight, (WORKERS, LANES))

    weights = [jnp.broadcast_to(bias[i : i + 1, :], (8, LANES)) for i in range(WORKERS)]

    def combine(t, carry):
        here = pl.ds(pl.multiple_of(t * 8, 8), 8)
        for q in range(held.shape[2] // LANES):
            there = slice(q * LANES, (q + 1) * LANES)
            sums = [weights[i] * held[i, here, there] for i in range(WORKERS)]
            while len(sums) > 1:
                sums = [a + b for a, b in zip(sums[::2], sums[1::2], strict=True)]
            out[here, there] = start[here, there] + sums[0]
        return carry

    lax.fori_loop(0, rows // 8, combine, 0, unroll=2)
    pltpu.make_async_copy(arrived, arrived, scalar_sent).wait()


def solution(mesh):
    def on_device(grads, center, radius):
        grads = grads.reshape(grads.shape[2], grads.shape[3])
        rows, columns = center.shape
        return pl.pallas_call(
            functools.partial(kernel, rows, rows // CHUNKS),
            out_shape=pltpu.VMEM((rows, columns), jnp.float32),
            in_specs=[pl.BlockSpec(memory_space=pltpu.HBM), pl.BlockSpec(memory_space=pltpu.HBM), pl.BlockSpec(memory_space=pltpu.SMEM)],
            out_specs=pl.BlockSpec(memory_space=pltpu.VMEM),
            scratch_shapes=[
                pltpu.VMEM((WORKERS, rows, columns), jnp.float32),
                pltpu.VMEM((rows, columns), jnp.float32),
                pltpu.VMEM((WORKERS * WORKERS, 8, LANES), jnp.float32),
                pltpu.VMEM((WORKERS, LANES), jnp.float32),
                pltpu.VMEM((2, LANES), jnp.float32),
                pltpu.VMEM((128, 2, LANES), jnp.float32),
                pltpu.VMEM((WORKERS * WORKERS, LANES), jnp.float32),
                pltpu.SemaphoreType.DMA,
                pltpu.SemaphoreType.DMA((CHUNKS,)),
                pltpu.SemaphoreType.DMA((2,)),
                pltpu.SemaphoreType.DMA,
                pltpu.SemaphoreType.DMA,
                pltpu.SemaphoreType.REGULAR((6,)),
            ],
            compiler_params=pltpu.CompilerParams(collective_id=0, has_side_effects=True, vmem_limit_bytes=60 * 2**20),
        )(grads, center, radius)

    return jax.shard_map(
        on_device,
        mesh=mesh,
        in_specs=(P("worker", "outer", None, "mp"), P(("worker", "outer"), "mp"), P()),
        out_specs=P(("worker", "outer"), "mp"),
        check_vma=False,
    )
```

```python
import functools
import math

import jax
import jax.numpy as jnp
from jax import lax
from jax.experimental import pallas as pl
from jax.experimental.pallas import tpu as pltpu
from jax.sharding import PartitionSpec as P

MESH = pl.DeviceIdType.MESH
D = 3584
KVW = 4096
WORKERS = 16
EPS = 1e-06
CHUNKS = 14
LANES = 128
BLOCK = 4


def far_devices():
    devices = [(x, y, z, c) for c in (0, 1) for x in range(4) for y in range(4) for z in range(4) if x or y or z or c]
    return sorted(devices, key=lambda d: (-sum(min(k, 4 - k) for k in d[:3]), -min(d[2], 4 - d[2])))


def kernel(rows, chunk, grads, center, radius, out, held, start, acc, bias, mine, every, lines, sent, landed, near, scalar_sent, scalar_landed, ready):
    w, o, m = lax.axis_index("worker"), lax.axis_index("outer"), lax.axis_index("mp")
    high, core = w // 2, w % 2
    me = w * 4 + o

    own = pltpu.make_async_copy(grads.at[pl.ds(pl.multiple_of(me * rows, 8), rows)], held.at[me], near.at[0])
    base = pltpu.make_async_copy(center, start, near.at[1])

    def device(x, flip, other, y_low=0, z=0):
        column = m // 4
        return ((high + flip) % 2) * 2 + (core + other) % 2, (o + x) % 4, ((column + y_low) % 2) * 4 + (m % 4 + z) % 4

    def greet(semaphore, *offsets):
        pl.semaphore_signal(semaphore, inc=1, device_id=device(*offsets), device_id_type=MESH)

    barrier = pltpu.get_barrier_semaphore()
    nearest = [(2, 0, 0), (0, 1, 0), (1, 0, 0), (3, 0, 0), (0, 0, 0, 0, 1), (0, 0, 0, 0, 3), (0, 0, 0, 1, 0), (0, 0, 1)]
    for offsets in nearest:
        greet(barrier, *offsets)
    own.start()
    base.start()
    pl.semaphore_wait(barrier, len(nearest))
    greet(ready.at[0], 0, 0, 1)
    greet(ready.at[1], 0, 1, 0)

    def to(offsets, c):
        worker, outer, part = device(*offsets)
        target = worker * 4 + outer
        at = pl.multiple_of(c * chunk, 8)
        pltpu.make_async_remote_copy(
            src_ref=grads.at[pl.ds(pl.multiple_of(target * rows + at, 8), chunk)],
            dst_ref=held.at[me, pl.ds(at, chunk)],
            send_sem=sent,
            recv_sem=landed.at[c],
            device_id=(worker, outer, part),
            device_id_type=MESH,
        ).start()

    def send(flip, h):
        for x in (1, 3, 2):
            to((x, flip, h % 2), h // 2)

        @pl.when(flip == 0)
        def _():
            to((0, 1, h % 2), h // 2)

    last = 2 * CHUNKS - 1
    send(0, 0)
    pl.semaphore_wait(ready.at[0], 1)

    @pl.when(core == 0)
    def _():
        send(0, 1)

    pl.semaphore_wait(ready.at[1], 1)
    greet(ready.at[2], 0, 0, 1)

    @pl.when(core == 1)
    def _():
        send(1, 0)

    pl.semaphore_wait(ready.at[2], 1)

    def partner(c, carry):
        to((0, 0, 1), c)
        return carry

    lax.fori_loop(0, CHUNKS, partner, 0)

    def turn(s, carry):
        before = s - 1
        send((before + core) % 2, core * (s // 2) + (1 - core) * (before // 2 + 1 - before % 2))
        return carry

    lax.fori_loop(2, 2 * last - 1, turn, 0)
    send(1, last - 1)
    send(1, last)
    send(0, last)

    greet(ready.at[3], 0, 0, 0, 1, 0)
    pl.semaphore_wait(ready.at[3], 1)
    greet(ready.at[4], 0, 0, 0, 0, 1)
    greet(ready.at[4], 0, 0, 0, 0, 3)
    pl.semaphore_wait(ready.at[4], 2)
    greet(ready.at[5], 0, 0, 0, 0, 3)
    pl.semaphore_wait(ready.at[5], 1)

    acc[...] = jnp.zeros_like(acc)
    own.wait()
    base.wait()

    def gather(c, carry):
        at = pl.multiple_of(c * chunk, 8)
        arrived = held.at[pl.ds(0, WORKERS - 1), pl.ds(at, chunk)]
        pltpu.make_async_copy(arrived, arrived, landed.at[c]).wait()

        def subtract(t, carry):
            here = pl.ds(pl.multiple_of(at + t * 8, 8), 8)
            v = start[here, :]
            for i in range(WORKERS):
                held[i, here, :] = held[i, here, :] - v
            return carry

        lax.fori_loop(0, chunk // 8, subtract, 0)
        for bi in range(WORKERS // BLOCK):
            for bj in range(bi, WORKERS // BLOCK):
                pairs = [(i, j) for i in range(bi * BLOCK, (bi + 1) * BLOCK) for j in range(bj * BLOCK, (bj + 1) * BLOCK) if i <= j]

                def products(t, sums, bi=bi, bj=bj, pairs=pairs):
                    here = pl.ds(pl.multiple_of(at + t * 8, 8), 8)
                    sums = list(sums)
                    for q in range(held.shape[2] // LANES):
                        there = slice(q * LANES, (q + 1) * LANES)
                        d = {i: held[i, here, there] for i in range(bi * BLOCK, (bi + 1) * BLOCK)}
                        for j in range(bj * BLOCK, (bj + 1) * BLOCK):
                            if j not in d:
                                d[j] = held[j, here, there]
                        for k, (i, j) in enumerate(pairs):
                            sums[k] = sums[k] + d[i] * d[j]
                    return tuple(sums)

                sums = lax.fori_loop(0, chunk // 8, products, tuple(acc[i * WORKERS + j] for i, j in pairs))
                for (i, j), total in zip(pairs, sums, strict=True):
                    acc[i * WORKERS + j] = total
        return carry

    lax.fori_loop(0, CHUNKS, gather, 0)

    def line(i, j):
        return (i // 8) * LANES + ((8 - i % 8) % 8) * WORKERS + j

    for i in range(WORKERS):
        for j in range(i, WORKERS):
            whole = jnp.sum(acc[i * WORKERS + j], axis=0, keepdims=True)
            for at in sorted({line(i, j), line(j, i)}):
                lines[at : at + 1, :] = whole
    across = lax.dot_general(
        jnp.full((8, LANES), 1.0, jnp.float32),
        lines[...] * 0.0625,
        (((1,), (1,)), ((), ())),
        precision=lax.Precision.HIGHEST,
        preferred_element_type=jnp.float32,
    )
    top = lax.broadcasted_iota(jnp.int32, (8, LANES), 0) == 0
    mine[...] = (jnp.where(top, across[:, :LANES], across[:, LANES:]) * 16.0)[0:2]

    y = high * 2 + m // 4
    slot = ((o * 4 + y) * 4 + m % 4) * 2 + core
    for dx, dy, dz, dc in far_devices():
        there = (y + dy) % 4
        pltpu.make_async_remote_copy(
            src_ref=mine, dst_ref=every.at[slot], send_sem=scalar_sent, recv_sem=scalar_landed,
            device_id=((there // 2) * 2 + (core + dc) % 2, (o + dx) % 4, (there % 2) * 4 + (m % 4 + dz) % 4),
            device_id_type=MESH,
        ).start()
    every[slot] = mine[...]
    pltpu.make_async_copy(held.at[pl.ds(0, WORKERS - 1)], held.at[pl.ds(0, WORKERS - 1)], sent).wait()
    arrived = every.at[pl.ds(0, 127)]
    pltpu.make_async_copy(arrived, arrived, scalar_landed).wait()
    total = jnp.sum(jnp.sum(every[...].reshape(16, 8, 2, LANES), axis=0), axis=0)

    tables = [
        pltpu.roll(jnp.broadcast_to(total[h : h + 1, :], (8, LANES)), 0, 1, stride=WORKERS, stride_axis=0) for h in (0, 1)
    ]
    gram = jnp.concatenate(tables, axis=0)
    row = lax.broadcasted_iota(jnp.int32, (WORKERS, LANES), 0)
    column = lax.broadcasted_iota(jnp.int32, (WORKERS, LANES), 1)
    tau = radius[0] * math.sqrt(D * KVW)

    def share(squares):
        return jnp.minimum(1.0, tau * lax.rsqrt(squares + EPS)) * (1.0 / WORKERS)

    diagonal = jnp.where(row == column, gram, 0.0)
    squares = jnp.sum(diagonal, axis=1, keepdims=True)
    squares = jnp.where(squares < jnp.inf, squares, jnp.inf)
    squares_row = jnp.sum(diagonal, axis=0, keepdims=True)
    squares_row = jnp.where(squares_row < jnp.inf, squares_row, jnp.inf)
    first = share(squares)
    first_row = share(squares_row)
    used = jnp.logical_and(column < WORKERS, first_row > 0.0)
    along = jnp.sum(jnp.where(used, first_row * gram, 0.0), axis=1, keepdims=True)
    moved = jnp.sum(jnp.where(first > 0.0, first * along, 0.0), axis=0, keepdims=True)
    again = jnp.maximum(squares - 2.0 * along + moved, 0.0)
    again = jnp.where(squares < jnp.inf, again, jnp.inf)
    second = share(again)
    weight = first * (1.0 - jnp.sum(second, axis=0, keepdims=True)) + second
    bias[...] = jnp.broadcast_to(weight, (WORKERS, LANES))

    weights = [jnp.broadcast_to(bias[i : i + 1, :], (8, LANES)) for i in range(WORKERS)]

    def combine(t, carry):
        here = pl.ds(pl.multiple_of(t * 8, 8), 8)
        for q in range(held.shape[2] // LANES):
            there = slice(q * LANES, (q + 1) * LANES)
            sums = [weights[i] * held[i, here, there] for i in range(WORKERS)]
            while len(sums) > 1:
                sums = [a + b for a, b in zip(sums[::2], sums[1::2], strict=True)]
            out[here, there] = start[here, there] + sums[0]
        return carry

    lax.fori_loop(0, rows // 8, combine, 0, unroll=2)
    pltpu.make_async_copy(arrived, arrived, scalar_sent).wait()


def solution(mesh):
    def on_device(grads, center, radius):
        grads = grads.reshape(grads.shape[2], grads.shape[3])
        rows, columns = center.shape
        return pl.pallas_call(
            functools.partial(kernel, rows, rows // CHUNKS),
            out_shape=pltpu.VMEM((rows, columns), jnp.float32),
            in_specs=[pl.BlockSpec(memory_space=pltpu.HBM), pl.BlockSpec(memory_space=pltpu.HBM), pl.BlockSpec(memory_space=pltpu.SMEM)],
            out_specs=pl.BlockSpec(memory_space=pltpu.VMEM),
            scratch_shapes=[
                pltpu.VMEM((WORKERS, rows, columns), jnp.float32),
                pltpu.VMEM((rows, columns), jnp.float32),
                pltpu.VMEM((WORKERS * WORKERS, 8, LANES), jnp.float32),
                pltpu.VMEM((WORKERS, LANES), jnp.float32),
                pltpu.VMEM((2, LANES), jnp.float32),
                pltpu.VMEM((128, 2, LANES), jnp.float32),
                pltpu.VMEM((WORKERS * WORKERS, LANES), jnp.float32),
                pltpu.SemaphoreType.DMA,
                pltpu.SemaphoreType.DMA((CHUNKS,)),
                pltpu.SemaphoreType.DMA((2,)),
                pltpu.SemaphoreType.DMA,
                pltpu.SemaphoreType.DMA,
                pltpu.SemaphoreType.REGULAR((6,)),
            ],
            compiler_params=pltpu.CompilerParams(collective_id=0, has_side_effects=True, vmem_limit_bytes=60 * 2**20),
        )(grads, center, radius)

    return jax.shard_map(
        on_device,
        mesh=mesh,
        in_specs=(P("worker", "outer", None, "mp"), P(("worker", "outer"), "mp"), P()),
        out_specs=P(("worker", "outer"), "mp"),
        check_vma=False,
    )
```
